32 devices in a mesh: rows: 8 (over z, x), cols: 4 (over y, core).
Axes of the slice: x: 2, y: 2, z: 4, core: 2. Of those that a mesh axis runs over, the one named last changes fastest.
Arguments:
- left_features: bfloat16 [2, 96, 512, 256], P(None, 'rows', 'cols'), may hold values from -6 to 6
- right_features: bfloat16 [2, 96, 512, 256], P(None, 'rows', 'cols'), may hold values from -6 to 6
- conv_weight: bfloat16 [3, 3, 256, 256], replicated, may hold values from -0.125 to 0.125
- conv_bias: float32 [256], replicated, may hold values from -3 to 3
Outputs:
- pyramid_out: float32 [2, 96, 512, 480], P(None, 'rows', 'cols')
The draws below stay inside these ranges and needn't reach their ends.
All inputs are finite; a program needn't handle non-finite values.
Results may differ from the reference program's by a relative error of at most 0.0012.
Values may be sent and summed in bfloat16 or wider, within the bound.
A program may use at most 64 MiB of HBM per device.

```python
import math
import jax
import jax.numpy as jnp
from jax import lax

C = 256
DISP = 256
LEVELS = 4
B = 2
H_FEAT = 96
W_FEAT = 512


def steps_of(own_key, dims, pieces, low, largest):
    loudness, own = 1.0, jax.random.fold_in(own_key, 6)
    for position, shards_of in pieces:
        heights = jnp.exp(jax.random.uniform(jax.random.fold_in(own, position), (shards_of,), jnp.float32, low / len(pieces), largest / len(pieces)))
        loudness = loudness * jnp.repeat(heights, dims[position] // shards_of).reshape([-1 if axis == position else 1 for axis in range(len(dims))])
    return loudness


def noise(stream_key, extent, spread, reach, pieces=(), held_as=jnp.bfloat16):
    values = spread * jax.random.normal(stream_key, extent, jnp.float32)
    if pieces:
        values = values * steps_of(stream_key, extent, pieces, -0.22, 0.18)
    return jnp.clip(values, -reach, reach).astype(held_as)


def setup_inputs(seed: int = 0) -> dict:
    seeds = jax.random.split(jax.random.key(seed), 5)
    left_features = noise(seeds[0], (B, H_FEAT, W_FEAT, C), 1.0, 6.0, ((1, 8), (2, 4)))
    right_features = noise(seeds[1], (B, H_FEAT, W_FEAT, C), 1.0, 6.0, ((1, 8), (2, 4)))
    conv_weight = noise(seeds[2], (3, 3, C, C), (9 * C) ** -0.5, 0.125)
    conv_bias = noise(seeds[3], (C,), 0.5, 3.0, (), jnp.float32)
    return {"left_features": left_features, "right_features": right_features, "conv_weight": conv_weight, "conv_bias": conv_bias}


def conv_block(picture, conv_weight, conv_bias):
    height = picture.shape[0] - 2
    breadth = picture.shape[1] - 2
    channels = picture.shape[2]
    total = jnp.zeros((height * breadth, channels), jnp.float32)
    for row_tap in range(3):
        for col_tap in range(3):
            window = picture[row_tap:row_tap + height, col_tap:col_tap + breadth].reshape(-1, channels)
            total = total + jnp.dot(window, conv_weight[row_tap, col_tap], preferred_element_type=jnp.float32)
    centre = picture[1:-1, 1:-1].reshape(-1, channels).astype(jnp.float32)
    encoded = centre + jax.nn.relu(total + conv_bias.astype(jnp.float32))
    return encoded.astype(jnp.bfloat16).reshape(height, breadth, channels)

def pyramid(scores, span_count, level_count, channels):
    queries = scores.shape[-2]
    across = scores.shape[-1]
    leading = scores.shape[:-2]
    skewed = scores[..., 1:].reshape(leading + (-1,))
    skewed = jnp.pad(skewed, [(0, 0)] * len(leading) + [(0, queries)])
    skewed = skewed.reshape(leading + (queries, across))[..., :span_count][..., ::-1]
    volume = skewed * (1.0 / math.sqrt(channels))
    levels = [volume]
    for level in range(1, level_count):
        pooled = volume.reshape(leading + (queries, span_count >> level, 1 << level)).mean(axis=-1)
        levels.append(pooled)
    return jnp.concatenate(levels, axis=-1)

def reference(left_features, right_features, conv_weight, conv_bias):
    batch, height, breadth, channels = left_features.shape

    def encode(images):
        padded = jnp.pad(images, ((0, 0), (1, 1), (1, 1), (0, 0)))
        return lax.map(lambda picture: conv_block(picture, conv_weight, conv_bias), padded)
    left_out = encode(left_features)
    right_out = encode(right_features)
    right_padded = jnp.pad(right_out, ((0, 0), (0, 0), (DISP, 0), (0, 0)))
    left_rows = left_out.reshape(batch * height, breadth, channels)
    right_rows = right_padded.reshape(batch * height, DISP + breadth, channels)

    def one_row(pair):
        scores = jnp.dot(pair[0], pair[1].T, preferred_element_type=jnp.float32)
        return pyramid(scores, DISP, LEVELS, channels)
    result = lax.map(one_row, (left_rows, right_rows))
    return result.reshape(batch, height, breadth, -1)
```

```python
import functools
import math

import jax
import jax.numpy as jnp
from jax import lax
from jax.experimental import pallas as pl
from jax.experimental.pallas import tpu as pltpu
from jax.sharding import PartitionSpec as P

DISP = 256
LEVELS = 4


def padded_2(cells, sides, width):
    for axis, dim in sides:
        count = lax.axis_size(axis)
        ends = count - 1
        head = lax.slice_in_dim(cells, 0, width, axis=dim)
        tail = lax.slice_in_dim(cells, cells.shape[dim] - width, cells.shape[dim], axis=dim)
        cells = jnp.concatenate(
            [
                lax.ppermute(tail, axis, [(i, (i + 1) % count) for i in range(ends)]),
                cells,
                lax.ppermute(head, axis, [((i + 1) % count, i) for i in range(ends)]),
            ],
            axis=dim,
        )
    return cells


def shifted(value, axis, steps):
    count = lax.axis_size(axis)
    leading, last = (max(0, -steps), min(count, count - steps))
    return lax.ppermute(value, axis, [(source, source + steps) for source in range(leading, last)])


def encode(padded, conv_weight, conv_bias):
    batch = padded.shape[0]
    height = padded.shape[1] - 2
    breadth = padded.shape[2] - 2
    channels = padded.shape[3]
    total = jnp.zeros((batch * height * breadth, channels), jnp.float32)
    for row_tap in range(3):
        for col_tap in range(3):
            window = padded[:, row_tap : row_tap + height, col_tap : col_tap + breadth].reshape(
                -1, channels
            )
            total = total + jnp.dot(
                window, conv_weight[row_tap, col_tap], preferred_element_type=jnp.float32
            )
    centre = padded[:, 1:-1, 1:-1].reshape(-1, channels).astype(jnp.float32)
    encoded = centre + jax.nn.relu(total + conv_bias)
    return encoded.astype(jnp.bfloat16).reshape(batch, height, breadth, channels)


def pooling(span_count, level_count):
    columns = []
    entry = lax.broadcasted_iota(jnp.int32, (span_count, 1), 0)
    for level in range(1, level_count):
        group = lax.broadcasted_iota(jnp.int32, (1, span_count >> level), 1)
        columns.append(jnp.where((entry >> level) == group, 0.5**level, 0.0))
    return jnp.concatenate(columns, axis=1).astype(jnp.bfloat16)


def correlate_kernel(span_count, scale, left_ref, *refs):
    right_refs, pool_ref, out_ref = refs[:-2], refs[-2], refs[-1]
    rows, breadth, _ = left_ref.shape
    across = breadth * len(right_refs)
    pool = pool_ref[...]
    for row in range(rows):
        query = left_ref[row]
        scores = jnp.concatenate(
            [
                lax.dot_general(
                    query, ref[row], (((1,), (1,)), ((), ())), preferred_element_type=jnp.float32
                )
                for ref in right_refs
            ],
            axis=1,
        )
        turned = pltpu.roll(scores, across - breadth + 1, 1, stride=1, stride_axis=0)
        volume = turned[:, :span_count] * scale
        high = volume.astype(jnp.bfloat16)
        low = (volume - high.astype(jnp.float32)).astype(jnp.bfloat16)
        pooled = jnp.dot(high, pool, preferred_element_type=jnp.float32) + jnp.dot(
            low, pool, preferred_element_type=jnp.float32
        )
        out_ref[row, :, :span_count] = volume
        out_ref[row, :, span_count:] = pooled


def correlate(left, rights, span_count, level_count, block):
    rows, breadth, channels = left.shape
    pool = pooling(span_count, level_count)
    width = span_count + pool.shape[1]
    part = pl.BlockSpec((block, breadth, channels), lambda i: (i, 0, 0))
    return pl.pallas_call(
        functools.partial(correlate_kernel, span_count, 1.0 / math.sqrt(channels)),
        grid=(rows // block,),
        out_shape=jax.ShapeDtypeStruct((rows, breadth, width), jnp.float32),
        in_specs=[part] * (1 + len(rights)) + [pl.BlockSpec(pool.shape, lambda i: (0, 0))],
        out_specs=pl.BlockSpec((block, breadth, width), lambda i: (i, 0, 0)),
        cost_estimate=pl.CostEstimate(
            flops=2 * rows * breadth * (len(rights) * breadth * channels + 2 * span_count * 256),
            bytes_accessed=rows * breadth * (2 * channels * (1 + len(rights)) + 4 * width),
            transcendentals=0,
        ),
    )(left, *rights, pool)


def shards(left_features, right_features, conv_weight, conv_bias):
    batch, height, breadth, channels = left_features.shape
    left_pad, right_pad = (
        padded_2(left_features, (("rows", 1), ("cols", 2)), 1),
        padded_2(right_features, (("rows", 1), ("cols", 2)), 1),
    )
    left_out = encode(left_pad, conv_weight, conv_bias)
    right_out = encode(right_pad, conv_weight, conv_bias)
    right_out = right_out[:, :, ::-1]
    hops = DISP // breadth
    count = lax.axis_size("cols")
    if hops == 2 and count % 2 == 0:
        far = shifted(right_out, "cols", 2)
        pairs = range(0, count, 2)
        own = lax.ppermute(right_out, "cols", [(i, i + 1) for i in pairs])
        back = lax.ppermute(far, "cols", [(i + 1, i) for i in pairs])
        odd = lax.rem(lax.axis_index("cols"), 2) == 1
        pieces = [right_out, jnp.where(odd, own, back), far]
    else:
        pieces = [right_out] + [shifted(right_out, "cols", step) for step in range(1, hops + 1)]
    rows_total = batch * height
    flat = [piece.reshape(rows_total, breadth, channels) for piece in pieces]
    out = correlate(
        left_out.reshape(rows_total, breadth, channels), flat, DISP, LEVELS, math.gcd(rows_total, 4)
    )
    return out.reshape(batch, height, breadth, -1)


def solution(mesh):
    return jax.shard_map(
        shards,
        mesh=mesh,
        in_specs=(P(None, "rows", "cols", None), P(None, "rows", "cols", None), P(), P()),
        out_specs=P(None, "rows", "cols", None),
        check_vma=False,
    )
```

```python
import functools
import math

import jax
import jax.numpy as jnp
from jax import lax
from jax.experimental import pallas as pl
from jax.experimental.pallas import tpu as pltpu
from jax.sharding import PartitionSpec as P

DISP = 256
LEVELS = 4


def padded_2(cells, sides, width):
    for axis, dim in sides:
        count = lax.axis_size(axis)
        ends = count - 1
        head = lax.slice_in_dim(cells, 0, width, axis=dim)
        tail = lax.slice_in_dim(cells, cells.shape[dim] - width, cells.shape[dim], axis=dim)
        cells = jnp.concatenate(
            [
                lax.ppermute(tail, axis, [(i, (i + 1) % count) for i in range(ends)]),
                cells,
                lax.ppermute(head, axis, [((i + 1) % count, i) for i in range(ends)]),
            ],
            axis=dim,
        )
    return cells


def shifted(value, axis, steps):
    count = lax.axis_size(axis)
    leading, last = (max(0, -steps), min(count, count - steps))
    return lax.ppermute(value, axis, [(source, source + steps) for source in range(leading, last)])


def encode(padded, conv_weight, conv_bias):
    batch = padded.shape[0]
    height = padded.shape[1] - 2
    breadth = padded.shape[2] - 2
    channels = padded.shape[3]
    total = jnp.zeros((batch * height * breadth, channels), jnp.float32)
    for row_tap in range(3):
        for col_tap in range(3):
            window = padded[:, row_tap : row_tap + height, col_tap : col_tap + breadth].reshape(
                -1, channels
            )
            total = total + jnp.dot(
                window, conv_weight[row_tap, col_tap], preferred_element_type=jnp.float32
            )
    centre = padded[:, 1:-1, 1:-1].reshape(-1, channels).astype(jnp.float32)
    encoded = centre + jax.nn.relu(total + conv_bias)
    return encoded.astype(jnp.bfloat16).reshape(batch, height, breadth, channels)


def pooling(span_count, level_count):
    lines = []
    entry = lax.broadcasted_iota(jnp.int32, (1, span_count), 1)
    for level in range(1, level_count):
        group = lax.broadcasted_iota(jnp.int32, (span_count >> level, 1), 0)
        lines.append(jnp.where((entry >> level) == group, 0.5**level, 0.0))
    return jnp.concatenate(lines, axis=0).astype(jnp.bfloat16)


def skewed(scores, span_count, scratch):
    breadth = scores.shape[1]
    lane = lax.broadcasted_iota(jnp.int32, (1, breadth), 1)
    steps = breadth - 1 - lane
    bit = breadth // 2
    while bit >= 8:
        keep = span_count + bit
        scores = jnp.where((steps & bit) != 0, scores[bit : bit + keep], scores[:keep])
        bit //= 2
    for stage, bit in enumerate((4, 2, 1)):
        keep = span_count + (8 if bit > 1 else 0)
        scratch[stage, : span_count + 8] = scores
        scores = jnp.where((steps & bit) != 0, scratch[stage, pl.ds(bit, keep)], scores[:keep])
    return scores


def correlate_kernel(span_count, scale, left_ref, *refs):
    right_refs, pool_ref, out_ref, scratch = refs[:-3], refs[-3], refs[-2], refs[-1]
    rows = left_ref.shape[0]
    pool = pool_ref[...]
    breadth = left_ref.shape[1]
    for pair in range(0, rows, 2):
        volumes = []
        for row in range(pair, min(pair + 2, rows)):
            query = left_ref[row]
            scores = jnp.concatenate(
                [
                    lax.dot_general(
                        ref[row], query, (((1,), (1,)), ((), ())), preferred_element_type=jnp.float32
                    )
                    for ref in right_refs
                ],
                axis=0,
            )
            volume = skewed(scores, span_count, scratch.at[row]) * scale
            out_ref[row, :span_count] = volume
            volumes.append(volume)
        volume = jnp.concatenate(volumes, axis=1)
        high = volume.astype(jnp.bfloat16)
        low = (volume - high.astype(jnp.float32)).astype(jnp.bfloat16)
        pooled = jnp.dot(pool, high, preferred_element_type=jnp.float32) + jnp.dot(
            pool, low, preferred_element_type=jnp.float32
        )
        for index in range(len(volumes)):
            out_ref[pair + index, span_count:] = pooled[:, index * breadth : (index + 1) * breadth]


def correlate(left, rights, span_count, level_count, block):
    rows, breadth, channels = left.shape
    pool = pooling(span_count, level_count)
    width = span_count + pool.shape[0]
    part = pl.BlockSpec((block, breadth, channels), lambda i: (i, 0, 0))
    return pl.pallas_call(
        functools.partial(correlate_kernel, span_count, 1.0 / math.sqrt(channels)),
        grid=(rows // block,),
        out_shape=jax.ShapeDtypeStruct((rows, width, breadth), jnp.float32),
        in_specs=[part] * (1 + len(rights)) + [pl.BlockSpec(pool.shape, lambda i: (0, 0))],
        out_specs=pl.BlockSpec((block, width, breadth), lambda i: (i, 0, 0)),
        scratch_shapes=[pltpu.VMEM((block, 3, span_count + 16, breadth), jnp.float32)],
        cost_estimate=pl.CostEstimate(
            flops=2 * rows * breadth * (len(rights) * breadth * channels + 2 * span_count * 256),
            bytes_accessed=rows * breadth * (2 * channels * (1 + len(rights)) + 4 * width),
            transcendentals=0,
        ),
    )(left, *rights, pool)


def shards(left_features, right_features, conv_weight, conv_bias):
    batch, height, breadth, channels = left_features.shape
    left_pad, right_pad = (
        padded_2(left_features, (("rows", 1), ("cols", 2)), 1),
        padded_2(right_features, (("rows", 1), ("cols", 2)), 1),
    )
    left_out = encode(left_pad, conv_weight, conv_bias)
    right_out = encode(right_pad, conv_weight, conv_bias)
    flip = jnp.eye(breadth, dtype=jnp.bfloat16)[::-1]
    right_out = jnp.einsum("xy,bhyc->bhxc", flip, right_out)
    hops = DISP // breadth
    count = lax.axis_size("cols")
    if hops == 2 and count % 2 == 0:
        far = shifted(right_out, "cols", 2)
        pairs = range(0, count, 2)
        own = lax.ppermute(right_out, "cols", [(i, i + 1) for i in pairs])
        back = lax.ppermute(far, "cols", [(i + 1, i) for i in pairs])
        odd = lax.rem(lax.axis_index("cols"), 2) == 1
        pieces = [right_out, jnp.where(odd, own, back), far]
    else:
        pieces = [right_out] + [shifted(right_out, "cols", step) for step in range(1, hops + 1)]
    rows_total = batch * height
    flat = [piece.reshape(rows_total, breadth, channels) for piece in pieces]
    out = correlate(
        left_out.reshape(rows_total, breadth, channels), flat, DISP, LEVELS, math.gcd(rows_total, 4)
    )
    return jnp.swapaxes(out, 1, 2).reshape(batch, height, breadth, -1)


def solution(mesh):
    return jax.shard_map(
        shards,
        mesh=mesh,
        in_specs=(P(None, "rows", "cols", None), P(None, "rows", "cols", None), P(), P()),
        out_specs=P(None, "rows", "cols", None),
        check_vma=False,
    )
```

```python
import functools
import math

import jax
import jax.numpy as jnp
from jax import lax
from jax.experimental import pallas as pl
from jax.experimental.pallas import tpu as pltpu
from jax.sharding import PartitionSpec as P

DISP = 256
LEVELS = 4


MESH = pl.DeviceIdType.MESH
AROUND = ((-1, 0), (1, 0), (0, -1), (0, 1), (-1, -1), (-1, 1), (1, -1), (1, 1))
OPPOSITE = (1, 0, 3, 2, 7, 6, 5, 4)


def encode_kernel(
    row_count, col_count, part, images, row_edges, col_edges, corners, weight_ref, bias_ref, flip_ref,
    left_out, right_out, near, far,
    row_halo, col_halo, corner_halo, padded, send_sem, recv_sem, far_sems, own_sems, pass_sems
):
    _, batch, height, breadth, channels = images.shape
    my_row, my_col = lax.axis_index("rows"), lax.axis_index("cols")
    parts = height // part
    chunks = batch * parts

    def inside(step_row, step_col):
        row, col = my_row + step_row, my_col + step_col
        return (row >= 0) & (row < row_count) & (col >= 0) & (col < col_count)

    barrier = pltpu.get_barrier_semaphore()
    partners = AROUND + ((0, -2), (0, 2))
    for step_row, step_col in partners:

        @pl.when(inside(step_row, step_col))
        def _():
            pl.semaphore_signal(
                barrier, inc=1, device_id=(my_row + step_row, my_col + step_col), device_id_type=MESH
            )

    peers = sum(inside(*step).astype(jnp.int32) for step in partners)
    pl.semaphore_wait(barrier, peers)

    def halo(side):
        if side < 2:
            return row_edges.at[side], row_halo
        if side < 4:
            return col_edges.at[side - 2], col_halo
        return corners.at[side - 4], corner_halo

    def halo_copy(side):
        first = 0 if side < 2 else 2 if side < 4 else 4
        source, target = halo(side)
        there = OPPOSITE[side]
        return pltpu.make_async_remote_copy(
            src_ref=source, dst_ref=target.at[there - first],
            send_sem=send_sem.at[side], recv_sem=recv_sem.at[there],
            device_id=(my_row + AROUND[side][0], my_col + AROUND[side][1]), device_id_type=MESH,
        )

    for side in range(8):
        there = inside(*AROUND[side])

        @pl.when(there)
        def _():
            halo_copy(side).start()

        @pl.when(jnp.logical_not(there))
        def _():
            first = 0 if side < 2 else 2 if side < 4 else 4
            target = halo(side)[1]
            target[side - first] = jnp.zeros(target.shape[1:], target.dtype)

    has_far = my_col >= 2
    odd = lax.rem(my_col, 2) == 1
    has_near = odd | has_far

    @pl.when(jnp.logical_not(has_far))
    def _():
        far[...] = jnp.zeros_like(far)

    @pl.when(jnp.logical_not(has_near))
    def _():
        near[...] = jnp.zeros_like(near)

    for side in range(8):

        @pl.when(inside(*AROUND[OPPOSITE[side]]))
        def _():
            halo_copy(side).wait_recv()

    column = lax.broadcasted_iota(jnp.int32, (breadth, 1), 0)

    def place(image, b, line, row, before, after):
        wide = row.astype(jnp.float32)
        right = jnp.where(column == 0, before.astype(jnp.float32), pltpu.roll(wide, 1, 0))
        left = jnp.where(
            column == breadth - 1, after.astype(jnp.float32), pltpu.roll(wide, breadth - 1, 0)
        )
        padded[image, b, line] = jnp.concatenate(
            [right.astype(jnp.bfloat16), row, left.astype(jnp.bfloat16)], axis=1
        )

    def prepare(image):
        for b in range(batch):
            for edge in range(2):
                place(
                    image, b, edge * (height + 1), row_halo[edge, image, b],
                    corner_halo[2 * edge, image, b], corner_halo[2 * edge + 1, image, b],
                )

            def line(h, carry):
                place(
                    image, b, h + 1, images[image, b, h],
                    col_halo[0, image, b, h], col_halo[1, image, b, h],
                )
                return carry

            lax.fori_loop(0, height, line, 0)

    def encoded(image, b, h):
        total = bias_ref[...]
        for tap in range(3):
            window = padded[image, b, pl.ds(h + tap, part)].reshape(part * breadth, 3 * channels)
            product = jnp.dot(window, weight_ref[tap], preferred_element_type=jnp.float32)
            total = product + total
        centre = images[image, b, pl.ds(h, part)].reshape(part * breadth, channels)
        out = centre.astype(jnp.float32) + jnp.maximum(total, 0.0)
        return out.astype(jnp.bfloat16).reshape(part, breadth, channels)

    def far_copy(i):
        rows = pl.ds(i * part, part)
        return pltpu.make_async_remote_copy(
            src_ref=right_out.at[rows], dst_ref=far.at[rows],
            send_sem=far_sems.at[0, i], recv_sem=far_sems.at[1, i],
            device_id=(my_row, my_col + 2), device_id_type=MESH,
        )

    def own_copy(i):
        rows = pl.ds(i * part, part)
        return pltpu.make_async_remote_copy(
            src_ref=right_out.at[rows], dst_ref=near.at[rows],
            send_sem=own_sems.at[0, i], recv_sem=own_sems.at[1, i],
            device_id=(my_row, my_col + 1), device_id_type=MESH,
        )

    def pass_copy(i):
        rows = pl.ds(i * part, part)
        return pltpu.make_async_remote_copy(
            src_ref=far.at[rows], dst_ref=near.at[rows],
            send_sem=pass_sems.at[0, i], recv_sem=pass_sems.at[1, i],
            device_id=(my_row, my_col - 1), device_id_type=MESH,
        )

    sends_far = my_col + 2 < col_count
    even = jnp.logical_not(odd)
    prepare(1)

    def right_chunk(i, carry):
        enc = encoded(1, i // parts, (i % parts) * part)
        for row in range(part):
            turned = jnp.dot(flip_ref[...], enc[row], preferred_element_type=jnp.float32)
            right_out[i * part + row] = turned.astype(jnp.bfloat16)

        @pl.when(sends_far)
        def _():
            far_copy(i).start()

        @pl.when(even)
        def _():
            own_copy(i).start()

        return carry

    lax.fori_loop(0, chunks, right_chunk, 0)
    prepare(0)

    def left_chunk(i, carry):
        left_out[pl.ds(i * part, part)] = encoded(0, i // parts, (i % parts) * part)
        return carry

    lax.fori_loop(0, chunks, left_chunk, 0)

    def arrive(i, carry):
        @pl.when(has_far)
        def _():
            far_copy(i).wait_recv()

        @pl.when(has_far & odd)
        def _():
            pass_copy(i).start()

        return carry

    lax.fori_loop(0, chunks, arrive, 0)

    def finish(i, carry):
        @pl.when(odd)
        def _():
            own_copy(i).wait_recv()

        @pl.when(has_far & even)
        def _():
            pass_copy(i).wait_recv()

        @pl.when(has_far & odd)
        def _():
            pass_copy(i).wait_send()

        @pl.when(sends_far)
        def _():
            far_copy(i).wait_send()

        @pl.when(even)
        def _():
            own_copy(i).wait_send()

        return carry

    lax.fori_loop(0, chunks, finish, 0)
    for side in range(8):

        @pl.when(inside(*AROUND[side]))
        def _():
            halo_copy(side).wait_send()


def encode(left_features, right_features, conv_weight, conv_bias):
    batch, height, breadth, channels = left_features.shape
    images = jnp.stack([left_features, right_features])
    row_edges = jnp.stack([images[:, :, 0], images[:, :, -1]])
    col_edges = jnp.stack([images[:, :, :, :1], images[:, :, :, -1:]])
    corners = jnp.stack(
        [images[:, :, r, c : c + 1] for r in (0, height - 1) for c in (0, breadth - 1)]
    )
    weight = conv_weight.reshape(3, 3 * channels, channels)
    flip = jnp.eye(breadth, dtype=jnp.bfloat16)[::-1]
    part = math.gcd(height, 4)
    chunks = batch * height // part
    flat = jax.ShapeDtypeStruct((batch * height, breadth, channels), jnp.bfloat16)
    vmem = pl.BlockSpec(memory_space=pltpu.VMEM)
    dma = pltpu.SemaphoreType.DMA
    return pl.pallas_call(
        functools.partial(encode_kernel, lax.axis_size("rows"), lax.axis_size("cols"), part),
        out_shape=[flat] * 4,
        in_specs=[vmem] * 7,
        out_specs=[vmem] * 4,
        scratch_shapes=[
            pltpu.VMEM(row_edges.shape, jnp.bfloat16),
            pltpu.VMEM(col_edges.shape, jnp.bfloat16),
            pltpu.VMEM(corners.shape, jnp.bfloat16),
            pltpu.VMEM((2, batch, height + 2, breadth, 3 * channels), jnp.bfloat16),
            dma((8,)), dma((8,)), dma((2, chunks)), dma((2, chunks)), dma((2, chunks)),
        ],
        compiler_params=pltpu.CompilerParams(
            collective_id=0, has_side_effects=True, vmem_limit_bytes=60 * 2**20
        ),
    )(images, row_edges, col_edges, corners, weight, conv_bias.reshape(1, -1), flip)


def pooling(span_count, level_count):
    lines = []
    entry = lax.broadcasted_iota(jnp.int32, (1, span_count), 1)
    for level in range(1, level_count):
        group = lax.broadcasted_iota(jnp.int32, (span_count >> level, 1), 0)
        lines.append(jnp.where((entry >> level) == group, 0.5**level, 0.0))
    return jnp.concatenate(lines, axis=0).astype(jnp.bfloat16)


def skewed(scores, span_count, scratch):
    breadth = scores.shape[1]
    lane = lax.broadcasted_iota(jnp.int32, (1, breadth), 1)
    steps = breadth - 1 - lane
    bit = breadth // 2
    while bit >= 8:
        keep = span_count + bit
        scores = jnp.where((steps & bit) != 0, scores[bit : bit + keep], scores[:keep])
        bit //= 2
    for stage, bit in enumerate((4, 2, 1)):
        keep = span_count + (8 if bit > 1 else 0)
        scratch[stage, : span_count + 8] = scores
        scores = jnp.where((steps & bit) != 0, scratch[stage, pl.ds(bit, keep)], scores[:keep])
    return scores


def correlate_kernel(span_count, scale, left_ref, *refs):
    right_refs, pool_ref, out_ref, scratch = refs[:-3], refs[-3], refs[-2], refs[-1]
    rows = left_ref.shape[0]
    pool = pool_ref[...]
    breadth = left_ref.shape[1]
    for pair in range(0, rows, 2):
        volumes = []
        for row in range(pair, min(pair + 2, rows)):
            query = left_ref[row]
            scores = jnp.concatenate(
                [
                    lax.dot_general(
                        ref[row], query, (((1,), (1,)), ((), ())), preferred_element_type=jnp.float32
                    )
                    for ref in right_refs
                ],
                axis=0,
            )
            volume = skewed(scores, span_count, scratch.at[row]) * scale
            out_ref[row, :span_count] = volume
            volumes.append(volume)
        volume = jnp.concatenate(volumes, axis=1)
        high = volume.astype(jnp.bfloat16)
        low = (volume - high.astype(jnp.float32)).astype(jnp.bfloat16)
        pooled = jnp.dot(pool, high, preferred_element_type=jnp.float32) + jnp.dot(
            pool, low, preferred_element_type=jnp.float32
        )
        for index in range(len(volumes)):
            out_ref[pair + index, span_count:] = pooled[:, index * breadth : (index + 1) * breadth]


def correlate(left, rights, span_count, level_count, block):
    rows, breadth, channels = left.shape
    pool = pooling(span_count, level_count)
    width = span_count + pool.shape[0]
    part = pl.BlockSpec((block, breadth, channels), lambda i: (i, 0, 0))
    return pl.pallas_call(
        functools.partial(correlate_kernel, span_count, 1.0 / math.sqrt(channels)),
        grid=(rows // block,),
        out_shape=jax.ShapeDtypeStruct((rows, width, breadth), jnp.float32),
        in_specs=[part] * (1 + len(rights)) + [pl.BlockSpec(pool.shape, lambda i: (0, 0))],
        out_specs=pl.BlockSpec((block, width, breadth), lambda i: (i, 0, 0)),
        scratch_shapes=[pltpu.VMEM((block, 3, span_count + 16, breadth), jnp.float32)],
        cost_estimate=pl.CostEstimate(
            flops=2 * rows * breadth * (len(rights) * breadth * channels + 2 * span_count * 256),
            bytes_accessed=rows * breadth * (2 * channels * (1 + len(rights)) + 4 * width),
            transcendentals=0,
        ),
    )(left, *rights, pool)


def shards(left_features, right_features, conv_weight, conv_bias):
    batch, height, breadth, channels = left_features.shape
    count = lax.axis_size("cols")
    assert 2 * breadth == DISP and count % 2 == 0
    left, right, near, far = encode(left_features, right_features, conv_weight, conv_bias)
    rows_total = batch * height
    out = correlate(left, [right, near, far], DISP, LEVELS, math.gcd(rows_total, 4))
    return jnp.swapaxes(out, 1, 2).reshape(batch, height, breadth, -1)


def solution(mesh):
    return jax.shard_map(
        shards,
        mesh=mesh,
        in_specs=(P(None, "rows", "cols", None), P(None, "rows", "cols", None), P(), P()),
        out_specs=P(None, "rows", "cols", None),
        check_vma=False,
    )
```

```python
import functools
import math

import jax
import jax.numpy as jnp
import numpy as np
from jax import lax
from jax.experimental import pallas as pl
from jax.experimental.pallas import tpu as pltpu
from jax.sharding import PartitionSpec as P

DISP = 256
LEVELS = 4


MESH = pl.DeviceIdType.MESH
AROUND = ((-1, 0), (1, 0), (0, -1), (0, 1), (-1, -1), (-1, 1), (1, -1), (1, 1))
OPPOSITE = (1, 0, 3, 2, 7, 6, 5, 4)


def encode_kernel(
    row_count, col_count, part, left_in, right_in, row_edges, col_edges, corners, weight_ref, bias_ref, flip_ref,
    left_out, right_out, near, far,
    row_halo, col_halo, corner_halo, padded, send_sem, recv_sem, far_sems, own_sems, pass_sems
):
    batch, height, breadth, channels = left_in.shape
    images = (left_in, right_in)
    my_row, my_col = lax.axis_index("rows"), lax.axis_index("cols")
    parts = height // part
    chunks = batch * parts

    def inside(step_row, step_col):
        row, col = my_row + step_row, my_col + step_col
        return (row >= 0) & (row < row_count) & (col >= 0) & (col < col_count)

    barrier = pltpu.get_barrier_semaphore()
    partners = AROUND + ((0, -2), (0, 2))
    for step_row, step_col in partners:

        @pl.when(inside(step_row, step_col))
        def _():
            pl.semaphore_signal(
                barrier, inc=1, device_id=(my_row + step_row, my_col + step_col), device_id_type=MESH
            )

    peers = sum(inside(*step).astype(jnp.int32) for step in partners)
    pl.semaphore_wait(barrier, peers)

    def halo(side):
        if side < 2:
            return row_edges.at[side], row_halo
        if side < 4:
            return col_edges.at[side - 2], col_halo
        return corners.at[side - 4], corner_halo

    def halo_copy(side):
        first = 0 if side < 2 else 2 if side < 4 else 4
        source, target = halo(side)
        there = OPPOSITE[side]
        return pltpu.make_async_remote_copy(
            src_ref=source, dst_ref=target.at[there - first],
            send_sem=send_sem.at[side], recv_sem=recv_sem.at[there],
            device_id=(my_row + AROUND[side][0], my_col + AROUND[side][1]), device_id_type=MESH,
        )

    for side in range(8):
        there = inside(*AROUND[side])

        @pl.when(there)
        def _():
            halo_copy(side).start()

        @pl.when(jnp.logical_not(there))
        def _():
            first = 0 if side < 2 else 2 if side < 4 else 4
            target = halo(side)[1]
            target[side - first] = jnp.zeros(target.shape[1:], target.dtype)

    has_far = my_col >= 2
    odd = lax.rem(my_col, 2) == 1
    has_near = odd | has_far

    @pl.when(jnp.logical_not(has_far))
    def _():
        far[...] = jnp.zeros_like(far)

    @pl.when(jnp.logical_not(has_near))
    def _():
        near[...] = jnp.zeros_like(near)

    for side in range(8):

        @pl.when(inside(*AROUND[OPPOSITE[side]]))
        def _():
            halo_copy(side).wait_recv()

    column = lax.broadcasted_iota(jnp.int32, (breadth, 1), 0)

    def place(image, b, line, row, before, after):
        wide = row.astype(jnp.float32)
        right = jnp.where(column == 0, before.astype(jnp.float32), pltpu.roll(wide, 1, 0))
        left = jnp.where(
            column == breadth - 1, after.astype(jnp.float32), pltpu.roll(wide, breadth - 1, 0)
        )
        padded[image, b, line] = jnp.concatenate(
            [right.astype(jnp.bfloat16), row, left.astype(jnp.bfloat16)], axis=1
        )

    def prepare(image):
        for b in range(batch):
            for edge in range(2):
                place(
                    image, b, edge * (height + 1), row_halo[edge, image, b],
                    corner_halo[2 * edge, image, b], corner_halo[2 * edge + 1, image, b],
                )

            def line(h, carry):
                place(
                    image, b, h + 1, images[image][b, h],
                    col_halo[0, image, b, h], col_halo[1, image, b, h],
                )
                return carry

            lax.fori_loop(0, height, line, 0)

    def encoded(image, b, h):
        total = bias_ref[...]
        for tap in range(3):
            window = padded[image, b, pl.ds(h + tap, part)].reshape(part * breadth, 3 * channels)
            product = jnp.dot(window, weight_ref[tap], preferred_element_type=jnp.float32)
            total = product + total
        centre = images[image][b, pl.ds(h, part)].reshape(part * breadth, channels)
        out = centre.astype(jnp.float32) + jnp.maximum(total, 0.0)
        return out.astype(jnp.bfloat16).reshape(part, breadth, channels)

    def far_copy(i):
        rows = pl.ds(i * part, part)
        return pltpu.make_async_remote_copy(
            src_ref=right_out.at[rows], dst_ref=far.at[rows],
            send_sem=far_sems.at[0, i], recv_sem=far_sems.at[1, i],
            device_id=(my_row, my_col + 2), device_id_type=MESH,
        )

    def own_copy(i):
        rows = pl.ds(i * part, part)
        return pltpu.make_async_remote_copy(
            src_ref=right_out.at[rows], dst_ref=near.at[rows],
            send_sem=own_sems.at[0, i], recv_sem=own_sems.at[1, i],
            device_id=(my_row, my_col + 1), device_id_type=MESH,
        )

    def pass_copy(i):
        rows = pl.ds(i * part, part)
        return pltpu.make_async_remote_copy(
            src_ref=far.at[rows], dst_ref=near.at[rows],
            send_sem=pass_sems.at[0, i], recv_sem=pass_sems.at[1, i],
            device_id=(my_row, my_col - 1), device_id_type=MESH,
        )

    sends_far = my_col + 2 < col_count
    even = jnp.logical_not(odd)
    prepare(1)

    def right_chunk(i, carry):
        enc = encoded(1, i // parts, (i % parts) * part)
        for row in range(part):
            turned = jnp.dot(flip_ref[...], enc[row], preferred_element_type=jnp.float32)
            right_out[i * part + row] = turned.astype(jnp.bfloat16)

        @pl.when(sends_far)
        def _():
            far_copy(i).start()

        @pl.when(even)
        def _():
            own_copy(i).start()

        return carry

    lax.fori_loop(0, chunks, right_chunk, 0)
    prepare(0)

    def left_chunk(i, carry):
        left_out[pl.ds(i * part, part)] = encoded(0, i // parts, (i % parts) * part)
        return carry

    lax.fori_loop(0, chunks, left_chunk, 0)

    def arrive(i, carry):
        @pl.when(has_far)
        def _():
            far_copy(i).wait_recv()

        @pl.when(has_far & odd)
        def _():
            pass_copy(i).start()

        return carry

    lax.fori_loop(0, chunks, arrive, 0)

    def finish(i, carry):
        @pl.when(odd)
        def _():
            own_copy(i).wait_recv()

        @pl.when(has_far & even)
        def _():
            pass_copy(i).wait_recv()

        @pl.when(has_far & odd)
        def _():
            pass_copy(i).wait_send()

        @pl.when(sends_far)
        def _():
            far_copy(i).wait_send()

        @pl.when(even)
        def _():
            own_copy(i).wait_send()

        return carry

    lax.fori_loop(0, chunks, finish, 0)
    for side in range(8):

        @pl.when(inside(*AROUND[side]))
        def _():
            halo_copy(side).wait_send()


def encode(left_features, right_features, conv_weight, conv_bias):
    batch, height, breadth, channels = left_features.shape
    pair = (left_features, right_features)
    row_edges = jnp.stack([jnp.stack([image[:, r] for image in pair]) for r in (0, -1)])
    col_edges = jnp.stack(
        [
            jnp.stack([image[:, :, c : c + 1] for image in pair])
            for c in (0, breadth - 1)
        ]
    )
    corners = jnp.stack(
        [
            jnp.stack([image[:, r, c : c + 1] for image in pair])
            for r in (0, height - 1)
            for c in (0, breadth - 1)
        ]
    )
    weight = conv_weight.reshape(3, 3 * channels, channels)
    flip = jnp.asarray(np.eye(breadth)[::-1], dtype=jnp.bfloat16)
    part = math.gcd(height, 4)
    chunks = batch * height // part
    flat = jax.ShapeDtypeStruct((batch * height, breadth, channels), jnp.bfloat16)
    vmem = pl.BlockSpec(memory_space=pltpu.VMEM)
    dma = pltpu.SemaphoreType.DMA
    return pl.pallas_call(
        functools.partial(encode_kernel, lax.axis_size("rows"), lax.axis_size("cols"), part),
        out_shape=[flat] * 4,
        in_specs=[vmem] * 8,
        out_specs=[vmem] * 4,
        scratch_shapes=[
            pltpu.VMEM(row_edges.shape, jnp.bfloat16),
            pltpu.VMEM(col_edges.shape, jnp.bfloat16),
            pltpu.VMEM(corners.shape, jnp.bfloat16),
            pltpu.VMEM((2, batch, height + 2, breadth, 3 * channels), jnp.bfloat16),
            dma((8,)), dma((8,)), dma((2, chunks)), dma((2, chunks)), dma((2, chunks)),
        ],
        compiler_params=pltpu.CompilerParams(
            collective_id=0, has_side_effects=True, vmem_limit_bytes=60 * 2**20
        ),
    )(left_features, right_features, row_edges, col_edges, corners, weight, conv_bias.reshape(1, -1), flip)


def pooling(span_count, level_count):
    lines = []
    entry = np.arange(span_count)[None, :]
    for level in range(1, level_count):
        group = np.arange(span_count >> level)[:, None]
        lines.append(np.where((entry >> level) == group, 0.5**level, 0.0))
    return jnp.asarray(np.concatenate(lines, axis=0), dtype=jnp.bfloat16)


def skewed(scores, span_count, scratch):
    breadth = scores.shape[1]
    lane = lax.broadcasted_iota(jnp.int32, (1, breadth), 1)
    steps = breadth - 1 - lane
    bit = breadth // 2
    while bit >= 8:
        keep = span_count + bit
        scores = jnp.where((steps & bit) != 0, scores[bit : bit + keep], scores[:keep])
        bit //= 2
    for stage, bit in enumerate((4, 2, 1)):
        keep = span_count + (8 if bit > 1 else 0)
        scratch[stage, : span_count + 8] = scores
        scores = jnp.where((steps & bit) != 0, scratch[stage, pl.ds(bit, keep)], scores[:keep])
    return scores


def correlate_kernel(span_count, scale, left_ref, *refs):
    right_refs, pool_ref, out_ref, scratch = refs[:-3], refs[-3], refs[-2], refs[-1]
    rows = left_ref.shape[0]
    pool = pool_ref[...]
    breadth = left_ref.shape[1]
    for pair in range(0, rows, 2):
        volumes = []
        for row in range(pair, min(pair + 2, rows)):
            query = left_ref[row]
            scores = jnp.concatenate(
                [
                    lax.dot_general(
                        ref[row], query, (((1,), (1,)), ((), ())), preferred_element_type=jnp.float32
                    )
                    for ref in right_refs
                ],
                axis=0,
            )
            volume = skewed(scores, span_count, scratch.at[row]) * scale
            out_ref[row, :span_count] = volume
            volumes.append(volume)
        volume = jnp.concatenate(volumes, axis=1)
        high = volume.astype(jnp.bfloat16)
        low = (volume - high.astype(jnp.float32)).astype(jnp.bfloat16)
        pooled = jnp.dot(pool, high, preferred_element_type=jnp.float32) + jnp.dot(
            pool, low, preferred_element_type=jnp.float32
        )
        for index in range(len(volumes)):
            out_ref[pair + index, span_count:] = pooled[:, index * breadth : (index + 1) * breadth]


def correlate(left, rights, span_count, level_count, block):
    rows, breadth, channels = left.shape
    pool = pooling(span_count, level_count)
    width = span_count + pool.shape[0]
    part = pl.BlockSpec((block, breadth, channels), lambda i: (i, 0, 0))
    return pl.pallas_call(
        functools.partial(correlate_kernel, span_count, 1.0 / math.sqrt(channels)),
        grid=(rows // block,),
        out_shape=jax.ShapeDtypeStruct((rows, width, breadth), jnp.float32),
        in_specs=[part] * (1 + len(rights)) + [pl.BlockSpec(pool.shape, lambda i: (0, 0))],
        out_specs=pl.BlockSpec((block, width, breadth), lambda i: (i, 0, 0)),
        scratch_shapes=[pltpu.VMEM((block, 3, span_count + 16, breadth), jnp.float32)],
        cost_estimate=pl.CostEstimate(
            flops=2 * rows * breadth * (len(rights) * breadth * channels + 2 * span_count * 256),
            bytes_accessed=rows * breadth * (2 * channels * (1 + len(rights)) + 4 * width),
            transcendentals=0,
        ),
    )(left, *rights, pool)


def shards(left_features, right_features, conv_weight, conv_bias):
    batch, height, breadth, channels = left_features.shape
    count = lax.axis_size("cols")
    assert 2 * breadth == DISP and count % 2 == 0
    left, right, near, far = encode(left_features, right_features, conv_weight, conv_bias)
    rows_total = batch * height
    out = correlate(left, [right, near, far], DISP, LEVELS, math.gcd(rows_total, 4))
    return jnp.swapaxes(out, 1, 2).reshape(batch, height, breadth, -1)


def solution(mesh):
    return jax.shard_map(
        shards,
        mesh=mesh,
        in_specs=(P(None, "rows", "cols", None), P(None, "rows", "cols", None), P(), P()),
        out_specs=P(None, "rows", "cols", None),
        check_vma=False,
    )
```
